256 devices in a mesh: heads: 4 (over y_hi, core), blk: 64 (over y_lo, z, x).
Axes of the slice: x: 4, y: 4 (y_hi: 2, y_lo: 2; y = y_hi * 2 + y_lo), z: 8, core: 2. Of those that a mesh axis runs over, the one named last changes fastest.
Arguments:
- tokens: bfloat16 [32768, 4096], P(('blk', 'heads')), may hold values from -6 to 6
- w_query: bfloat16 [4096, 2048], P('blk', 'heads'), may hold values from -0.75 to 0.75
- key_value_weight: bfloat16 [4096, 2, 512], P('blk', None, 'heads'), may hold values from -0.75 to 0.75
- w_out: bfloat16 [2048, 4096], P(('heads', 'blk')), may hold values from -0.5 to 0.5
- doc_lengths: int32 [16], replicated, may hold values from 1 to 8192, 32768 in all
Outputs:
- attended: bfloat16 [32768, 4096], P(('blk', 'heads'))
The draws below stay inside these ranges and needn't reach their ends.
Inputs may be any that keep to these rules, and one draw needn't show every extreme that they name: `doc_lengths`: the 16 lengths sum to 32768; the longest document has exactly 8192 tokens.
All inputs are finite; a program needn't handle non-finite values.
Results may differ from the reference program's by a relative error of at most 0.012.
Values may be sent and summed in bfloat16 or wider, within the bound.
A program may use at most 128 MiB of HBM per device.

```python
import math
import jax
import jax.numpy as jnp
import numpy as np
from jax import lax

MODEL_WIDTH = 4096
QUERY_HEADS = 16
KEY_VALUE_HEADS = 4
HEAD_SIZE = 128
NDOC = 16
PACK_TOKENS = 32768
BLOCK_TOKENS = 512
DOC_MAX = 8192
REACH = 16


def shared_weights(key):
    expand_heads = MODEL_WIDTH ** (-0.5)
    base_query = jax.random.truncated_normal(jax.random.fold_in(key, 11), -6.0, 6.0, (MODEL_WIDTH, QUERY_HEADS, HEAD_SIZE), jnp.float32) * expand_heads
    unrotated_keys = jax.random.truncated_normal(jax.random.fold_in(key, 12), -6.0, 6.0, (MODEL_WIDTH, KEY_VALUE_HEADS, HEAD_SIZE), jnp.float32) * expand_heads
    projected_values = jax.random.truncated_normal(jax.random.fold_in(key, 13), -6.0, 6.0, (MODEL_WIDTH, KEY_VALUE_HEADS, HEAD_SIZE), jnp.float32) * expand_heads
    key_matrix = unrotated_keys
    query_weights = base_query
    limit = 48.0 * expand_heads
    query_weights = jnp.clip(query_weights, -limit, limit).reshape(MODEL_WIDTH, QUERY_HEADS * HEAD_SIZE)
    key_value_matrix = jnp.stack([key_matrix.reshape(MODEL_WIDTH, KEY_VALUE_HEADS * HEAD_SIZE), projected_values.reshape(MODEL_WIDTH, KEY_VALUE_HEADS * HEAD_SIZE)], axis=1)
    key_value_matrix = jnp.clip(key_value_matrix, -limit, limit)
    return (query_weights, key_value_matrix)


def draw_w_query(key, part):
    return shared_weights(key)[0].astype(jnp.bfloat16)


def draw_key_value_weight(key, part):
    return shared_weights(key)[1].astype(jnp.bfloat16)


def draw_tokens(key, part):
    own_part = jax.random.normal(jax.random.fold_in(key, 21), (PACK_TOKENS, MODEL_WIDTH), jnp.float32)
    result = own_part
    return jnp.clip(result, -6.0, 6.0).astype(jnp.bfloat16)


def block_scale(own_key, dims, cuts, low, high):
    loudness = 1.0
    for position, blocks in cuts:
        steps = jax.random.uniform(jax.random.fold_in(jax.random.fold_in(own_key, 6), position), (blocks,), jnp.float32, low / len(cuts), high / len(cuts))
        loudness = loudness * jnp.repeat(jnp.exp(steps), dims[position] // blocks).reshape((-1,) + (1,) * (len(dims) - 1 - position))
    return loudness


def split_up(count, total, most, slope):
    weights = [(1 << 20) // math.isqrt(rank ** slope) + 1 for rank in range(2, count + 1)]
    surplus, holding = total - most - (count - 1), [1] * (count - 1)
    while surplus > 0:
        movable = [i for i in range(count - 1) if holding[i] < most]
        pool, budget = sum([weights[i] for i in movable]), surplus
        for i in movable:
            more = min(most - holding[i], max(1, budget * weights[i] // pool), surplus)
            holding[i] = holding[i] + more
            surplus = surplus - more
    return np.array([most] + holding)


def ragged_sizes(key, amount, total, most, slope):
    if amount == 2:
        one = jax.random.randint(key, (), max(1, total - most), min(most, total - 1) + 1)
        return jnp.stack([one, total - one])
    sizes = jnp.asarray(split_up(amount, total, most, slope), jnp.int32)
    twos = (amount - 1) // 2
    source_of, sink = sizes[1:1 + 2 * twos:2], sizes[2:2 + 2 * twos:2]
    room = jnp.minimum(source_of - 1, most - sink)
    passed = jax.random.randint(jax.random.fold_in(key, 1), (twos,), 0, 1 << 20) % (room + 1)
    sizes = sizes.at[1:1 + 2 * twos:2].set(source_of - passed).at[2:2 + 2 * twos:2].set(sink + passed)
    return sizes[jax.random.permutation(jax.random.fold_in(key, 2), amount)]


def scatter_about(stream_key, shape, scale, most, split=(), kind=jnp.bfloat16):
    values = jax.random.normal(stream_key, shape, jnp.float32) * scale
    if len(split) > 0:
        values = block_scale(stream_key, shape, split, -0.22, 0.18) * values
    return jnp.clip(values, min=-most, max=most).astype(kind)


def setup_inputs(seed: int = 0) -> dict:
    keys = jax.random.split(jax.random.key(seed), 6)
    return {
        "tokens": draw_tokens(jax.random.fold_in(keys[5], 71), 0),
        "w_query": draw_w_query(jax.random.fold_in(keys[5], 71), 0),
        "key_value_weight": draw_key_value_weight(jax.random.fold_in(keys[5], 71), 0),
        "w_out": scatter_about(keys[3], (QUERY_HEADS * HEAD_SIZE, MODEL_WIDTH), HEAD_SIZE ** -0.5, 0.5, ((0, 256),)),
        "doc_lengths": ragged_sizes(keys[4], NDOC, PACK_TOKENS, DOC_MAX, 2).astype(jnp.int32),
    }


norm_epsilon = 1e-05
rope_base = 500000.0
masked_score = -1e+30

def locate_documents(positions, doc_lengths):
    ends = jnp.cumsum(doc_lengths).astype(jnp.int32)
    after = positions[:, None] >= ends[None, :]
    ident = lax.optimization_barrier(jnp.sum(after.astype(jnp.int32), axis=1))
    starts = lax.optimization_barrier(jnp.sum(jnp.where(after, doc_lengths[None, :], 0), axis=1)).astype(jnp.int32)
    return (ident, starts)

def apply_rotation(values, relative_offset):
    half = values.shape[-1] // 2
    freqs = jnp.power(rope_base, -2.0 * jnp.arange(half, dtype=jnp.float32) / values.shape[-1])
    angle = relative_offset.astype(jnp.float32)[:, None] * freqs[None, :]
    cosine = jnp.cos(angle)[:, None, :]
    sine = jnp.sin(angle)[:, None, :]
    first = values[..., :half]
    second = values[..., half:]
    return jnp.concatenate([first * cosine - second * sine, second * cosine + first * sine], axis=-1)

def reference(tokens, w_query, key_value_weight, w_out, doc_lengths):
    values = tokens.astype(jnp.float32)
    normalized_input = (values * lax.rsqrt(lax.optimization_barrier(jnp.mean(values * values, axis=1, keepdims=True)) + norm_epsilon)).astype(jnp.bfloat16)
    query_raw = jnp.dot(normalized_input, w_query, preferred_element_type=jnp.float32)
    key_value_projected = jnp.dot(normalized_input, key_value_weight.reshape(MODEL_WIDTH, 2 * KEY_VALUE_HEADS * HEAD_SIZE), preferred_element_type=jnp.float32)
    positions = jnp.arange(PACK_TOKENS, dtype=jnp.int32)
    ident, starts = locate_documents(positions, doc_lengths)
    relative_offset = positions - starts
    query_rows = apply_rotation(query_raw.reshape(PACK_TOKENS, QUERY_HEADS, HEAD_SIZE), relative_offset).astype(jnp.bfloat16)
    rotated_keys = apply_rotation(key_value_projected[:, :KEY_VALUE_HEADS * HEAD_SIZE].reshape(PACK_TOKENS, KEY_VALUE_HEADS, HEAD_SIZE), relative_offset).astype(jnp.bfloat16)
    value_rows = key_value_projected[:, KEY_VALUE_HEADS * HEAD_SIZE:].reshape(PACK_TOKENS, KEY_VALUE_HEADS, HEAD_SIZE).astype(jnp.bfloat16)
    front_offset = REACH * BLOCK_TOKENS
    window = (REACH + 1) * BLOCK_TOKENS
    padded_key_rows = jnp.concatenate([jnp.zeros((front_offset, KEY_VALUE_HEADS, HEAD_SIZE), jnp.bfloat16), rotated_keys], axis=0)
    padded_value_rows = jnp.concatenate([jnp.zeros((front_offset, KEY_VALUE_HEADS, HEAD_SIZE), jnp.bfloat16), value_rows], axis=0)
    head_group = QUERY_HEADS // KEY_VALUE_HEADS
    scale = HEAD_SIZE ** (-0.5)

    def one_block(block_index):
        leading_row = (block_index * BLOCK_TOKENS).astype(jnp.int32)
        query_block_rows = lax.dynamic_slice_in_dim(query_rows, leading_row, BLOCK_TOKENS, 0).reshape(BLOCK_TOKENS, KEY_VALUE_HEADS, head_group, HEAD_SIZE).astype(jnp.float32)
        key_block = lax.dynamic_slice_in_dim(padded_key_rows, leading_row, window, 0).astype(jnp.float32)
        value_block = lax.dynamic_slice_in_dim(padded_value_rows, leading_row, window, 0).astype(jnp.float32)
        query_pos = leading_row + jnp.arange(BLOCK_TOKENS, dtype=jnp.int32)
        key_pos = leading_row - front_offset + jnp.arange(window, dtype=jnp.int32)
        query_doc, unused_q = locate_documents(query_pos, doc_lengths)
        key_doc, unused_k = locate_documents(key_pos, doc_lengths)
        keep = (key_pos[None, :] >= 0) & (key_pos[None, :] <= query_pos[:, None]) & (key_doc[None, :] == query_doc[:, None])
        scores = jnp.einsum('qhgd,khd->hgqk', query_block_rows, key_block) * scale
        scores = jnp.where(keep, scores, masked_score)
        highest = lax.optimization_barrier(jnp.max(scores, axis=-1, keepdims=True))
        probs = jnp.where(keep, jnp.exp(scores - highest), 0.0)
        totals = lax.optimization_barrier(jnp.sum(probs, axis=-1))
        probs_b = lax.optimization_barrier(probs.astype(jnp.bfloat16))
        mixed = jnp.einsum('hgqk,khd->hgqd', probs_b.astype(jnp.float32), value_block)
        mixed = mixed / totals[..., None]
        return mixed.transpose(2, 0, 1, 3).reshape(BLOCK_TOKENS, QUERY_HEADS * HEAD_SIZE).astype(jnp.bfloat16)
    mixed_all = lax.map(one_block, jnp.arange(PACK_TOKENS // BLOCK_TOKENS, dtype=jnp.int32)).reshape(PACK_TOKENS, QUERY_HEADS * HEAD_SIZE)
    return jnp.dot(mixed_all, w_out, preferred_element_type=jnp.float32).astype(jnp.bfloat16)
```

```python
import functools

import jax
import jax.numpy as jnp
from jax import lax
from jax.experimental import pallas as pl
from jax.experimental.pallas import tpu as pltpu
from jax.sharding import PartitionSpec as P

MESH = pl.DeviceIdType.MESH
BF16 = jnp.bfloat16
F32 = jnp.float32

HEAD = 128
QH = 4
BLK = 512
PIECE = 128
WIDTH = 4096
NX, NZ, NYL = 4, 8, 2
norm_epsilon = 1e-05
rope_base = 500000.0
masked_score = -1e30
LOG2E = 1.4426950408889634


class Place:
    def __init__(self):
        h = lax.axis_index("heads")
        b = lax.axis_index("blk")
        self.h, self.b = h, b
        self.yh, self.c = lax.div(h, 2), lax.rem(h, 2)
        self.yl = lax.div(b, NX * NZ)
        self.z = lax.rem(lax.div(b, NX), NZ)
        self.x = lax.rem(b, NX)
        self.row = b - self.x
        self.xs = [lax.rem(self.x + k, NX) for k in range(NX)]
        self.zs = [lax.rem(self.z + k, NZ) for k in range(NZ)]
        self.xp = (h, self.row + self.xs[1])
        self.xm = (h, self.row + self.xs[3])
        base = b - self.z * NX
        self.zp = (h, base + self.zs[1] * NX)
        self.zm = (h, base + self.zs[7] * NX)
        self.yf = (h, lax.rem(b + NX * NZ, 2 * NX * NZ))
        self.core = (h + 1 - 2 * self.c, b)
        y = 2 * self.yh + self.yl
        inner = lax.rem(b, NX * NZ)
        self.yp = self.at_y(lax.rem(y + 1, 4), inner)
        self.ym = self.at_y(lax.rem(y + 3, 4), inner)
        self.far = lax.rem(h + 2, 4)
        self.nextrow = (h, lax.rem(b + NX, 64))
        self.prevrow = (h, lax.rem(b + 60, 64))

    def at_y(self, y, inner):
        return (2 * lax.div(y, 2) + self.c, NX * NZ * lax.rem(y, 2) + inner)


def meet(devices):
    barrier = pltpu.get_barrier_semaphore()
    for device in devices:
        pl.semaphore_signal(barrier, inc=1, device_id=device, device_id_type=MESH)
    pl.semaphore_wait(barrier, len(devices))


class Sends:
    def __init__(self, send_sem, recv_sem):
        self.send_sem, self.recv_sem, self.made = send_sem, recv_sem, []

    def start(self, src, dst, device):
        i = len(self.made)
        copy = pltpu.make_async_remote_copy(
            src_ref=src,
            dst_ref=dst,
            send_sem=self.send_sem.at[i],
            recv_sem=self.recv_sem.at[i],
            device_id=device,
            device_id_type=MESH,
        )
        copy.start()
        self.made.append(copy)
        return copy

    def same(self, ref, device):
        return self.start(ref, ref, device)

    def drain(self):
        for copy in self.made:
            copy.wait_send()


def project_kernel(
    tokens, wq_in, wkv_in, cos, sin, q_out, kv_out,
    xbuf, ra, rb, wq, wkv, acc, copy_sem, send_sem, recv_sem,
):
    p = Place()
    x, z, yl, h = p.x, p.z, p.yl, p.h
    own_q = pltpu.make_async_copy(wq_in, wq.at[yl, z, x], copy_sem.at[0])
    own_kv = pltpu.make_async_copy(wkv_in, wkv.at[yl, z, x], copy_sem.at[1])
    own_q.start()
    own_kv.start()
    meet([p.xp, p.xm, p.zp, p.zm, p.yp, p.ym, p.core])
    s = Sends(send_sem, recv_sem)
    own_kv.wait()
    y_kv = s.same(wkv.at[yl, z, x], p.yf)
    own_q.wait()
    y_q = s.same(wq.at[yl, z, x], p.yf)

    def normalize(i, carry):
        rows = pl.ds(pl.multiple_of(i * 16, 16), 16)
        v = tokens[rows, :].astype(F32)
        mean = jnp.mean(v * v, axis=1, keepdims=True)
        xbuf[h, rows, :] = (v * lax.rsqrt(mean + norm_epsilon)).astype(BF16)
        return carry

    lax.fori_loop(0, PIECE // 16, normalize, 0)

    y_kv.wait_recv()
    ax = (s.same(wkv.at[:, z, x], p.xp), s.same(wkv.at[:, z, x], p.xm))
    y_q.wait_recv()
    bz = (s.same(wq.at[:, z, x], p.zp), s.same(wq.at[:, z, x], p.zm))

    def bx_send(zz):
        return (s.same(wq.at[:, zz, x], p.xp), s.same(wq.at[:, zz, x], p.xm))

    def bx_forward(zz, pair):
        pair[0].wait_recv()
        one = s.same(wq.at[0, zz, p.xs[3]], p.xp)
        pair[1].wait_recv()
        return (one, s.same(wq.at[1, zz, p.xs[1]], p.xm))

    rows0 = bx_send(z)
    act_core = s.same(xbuf.at[h], p.core)
    act = (
        s.start(xbuf.at[h, pl.ds(0, 64)], ra, p.yp),
        s.start(xbuf.at[h, pl.ds(64, 64)], rb, p.ym),
    )

    def z_forward(buf, pair, step, pick):
        pair[0].wait_recv()
        pair[1].wait_recv()
        low, high = p.zs[NZ - step], p.zs[step]
        if step < NZ // 2 - 1:
            return (s.same(pick(buf, None, low), p.zp), s.same(pick(buf, None, high), p.zm))
        return (s.same(pick(buf, 0, low), p.zp), s.same(pick(buf, 1, high), p.zm))

    def pick_b(buf, part, zz):
        return buf.at[:, zz, x] if part is None else buf.at[part, zz, x]

    def pick_a(buf, part, zz):
        return buf.at[:, zz] if part is None else buf.at[part, zz]

    ax[0].wait_recv()
    ax_far0 = s.same(wkv.at[0, z, p.xs[3]], p.xp)
    ax[1].wait_recv()
    ax_far1 = s.same(wkv.at[1, z, p.xs[1]], p.xm)
    bz = z_forward(wq, bz, 1, pick_b)
    rows1 = (bx_send(p.zs[7]), bx_send(p.zs[1]))
    ax_far0.wait_recv()
    ax_far1.wait_recv()
    bz = z_forward(wq, bz, 2, pick_b)
    az = (s.same(pick_a(wkv, None, z), p.zp), s.same(pick_a(wkv, None, z), p.zm))
    rows2 = (bx_send(p.zs[6]), bx_send(p.zs[2]))
    far0 = bx_forward(z, rows0)
    act[0].wait_recv()
    hm = p.ym[0]
    hp = p.yp[0]
    relay0 = s.start(ra, xbuf.at[hm, pl.ds(0, 64)], p.yp)
    act[1].wait_recv()
    relay1 = s.start(rb, xbuf.at[hp, pl.ds(64, 64)], p.ym)
    bz = z_forward(wq, bz, 3, pick_b)
    rows3 = (bx_send(p.zs[5]), bx_send(p.zs[3]))
    far1 = (bx_forward(p.zs[7], rows1[0]), bx_forward(p.zs[1], rows1[1]))
    az = z_forward(wkv, az, 1, pick_a)
    bz[0].wait_recv()
    bz[1].wait_recv()
    rows4 = bx_send(p.zs[4])
    az = z_forward(wkv, az, 2, pick_a)
    far2 = (bx_forward(p.zs[6], rows2[0]), bx_forward(p.zs[2], rows2[1]))
    relay0.wait_recv()
    relay1.wait_recv()
    act_far = s.same(xbuf.at[p.far], p.core)
    az = z_forward(wkv, az, 3, pick_a)
    far3 = (bx_forward(p.zs[5], rows3[0]), bx_forward(p.zs[3], rows3[1]))
    far4 = bx_forward(p.zs[4], rows4)
    for pair in (az, far0, far1[0], far1[1], far2[0], far2[1], far3[0], far3[1], far4):
        pair[0].wait_recv()
        pair[1].wait_recv()
    act_core.wait_recv()
    act_far.wait_recv()

    def multiply(k, carry):
        left = xbuf[:, :, pl.ds(pl.multiple_of(k * 512, 512), 512)].reshape(BLK, 512)
        ky = lax.div(k, 4)
        kz = 2 * lax.rem(k, 4)
        right = wq[ky, pl.ds(kz, 2)].reshape(512, 512)
        acc[:, :512] += jnp.dot(left, right, preferred_element_type=F32)
        right = wkv[ky, pl.ds(kz, 2)].reshape(512, 256)
        acc[:, 512:] += jnp.dot(left, right, preferred_element_type=F32)
        return carry

    acc[...] = jnp.zeros_like(acc)
    lax.fori_loop(0, 8, multiply, 0)

    for t in range(4):
        rows = slice(t * PIECE, (t + 1) * PIECE)
        co, si = cos[rows, :], sin[rows, :]

        def rotated(at):
            v = acc[rows, at : at + HEAD]
            return v * co + pltpu.roll(v, HEAD // 2, 1) * si

        for j in range(QH):
            q_out[j, rows, :] = rotated(j * HEAD).astype(BF16)
        kv_out[:, rows] = rotated(QH * HEAD).T.astype(BF16)
        kv_out[:, BLK + t * PIECE : BLK + (t + 1) * PIECE] = acc[rows, 640:768].astype(BF16)
    s.drain()


def project(tokens, wq, wkv, cos, sin):
    vmem = pl.BlockSpec(memory_space=pltpu.VMEM)
    hbm = pl.BlockSpec(memory_space=pl.ANY)
    return pl.pallas_call(
        project_kernel,
        out_shape=(
            jax.ShapeDtypeStruct((QH, BLK, HEAD), BF16),
            jax.ShapeDtypeStruct((HEAD, 2 * BLK), BF16),
        ),
        in_specs=[vmem, hbm, hbm, vmem, vmem],
        out_specs=(vmem, vmem),
        scratch_shapes=[
            pltpu.VMEM((4, PIECE, WIDTH), BF16),
            pltpu.VMEM((64, WIDTH), BF16),
            pltpu.VMEM((64, WIDTH), BF16),
            pltpu.VMEM((NYL, NZ, NX, 64, 512), BF16),
            pltpu.VMEM((NYL, NZ, NX, 64, 256), BF16),
            pltpu.VMEM((BLK, 768), F32),
            pltpu.SemaphoreType.DMA((2,)),
            pltpu.SemaphoreType.DMA((64,)),
            pltpu.SemaphoreType.DMA((64,)),
        ],
        compiler_params=pltpu.CompilerParams(
            collective_id=1, has_side_effects=True, vmem_limit_bytes=48 << 20
        ),
        name="project",
    )(tokens, wq, wkv, cos, sin)


def attend_kernel(
    q, kv_in, start, wout_in, mixed, wout_out,
    kv, wout, acc, high, copy_sem, send_sem, recv_sem,
):
    p = Place()
    x, z, yl = p.x, p.z, p.yl
    own_kv = pltpu.make_async_copy(kv_in, kv.at[0, x], copy_sem.at[0])
    own_w = pltpu.make_async_copy(wout_in, wout.at[yl, z, x], copy_sem.at[1])
    own_kv.start()
    own_w.start()
    meet([p.xp, p.xm, p.zp, p.zm, p.yf, p.nextrow, p.prevrow])
    s = Sends(send_sem, recv_sem)
    factor = HEAD ** (-0.5) * LOG2E
    lane = lax.broadcasted_iota(jnp.int32, (256, BLK), 1)

    def attend(d, xx, diagonal=False):
        base = p.row * BLK + (xx - NX * d) * BLK
        keys = kv[d, xx, :, 0:BLK]
        vals = jnp.concatenate(
            [kv[d, xx, :, BLK + i * HEAD : BLK + (i + 1) * HEAD] for i in range(4)], axis=0
        )
        vals = jnp.concatenate([vals, jnp.ones((BLK, HEAD), BF16)], axis=1)

        def head(j, carry):
            for half in range(2):
                rows = slice(half * 256, half * 256 + 256)
                score = jnp.dot(q[j, rows, :], keys, preferred_element_type=F32) * factor
                first = start[rows, :] - base
                keep = lane >= jnp.concatenate([first] * 4, axis=1)
                if diagonal:
                    keep &= lane <= lax.broadcasted_iota(jnp.int32, (256, BLK), 0) + half * 256
                score = jnp.where(keep, score, masked_score)
                top = jnp.max(score, axis=1, keepdims=True)
                if diagonal:
                    new = jnp.broadcast_to(top, (256, HEAD))
                else:
                    old = high[j, rows, :]
                    new = jnp.maximum(old, top)
                probs = jnp.exp2(score - jnp.concatenate([new] * 4, axis=1)).astype(BF16)
                update = jnp.dot(probs, vals, preferred_element_type=F32)
                if not diagonal:
                    fade = jnp.exp2(old - new)
                    update += acc[j, rows, :] * jnp.concatenate([fade, fade], axis=1)
                acc[j, rows, :] = update
                high[j, rows, :] = new
            return carry

        lax.fori_loop(0, QH, head, 0)

    def both(ref):
        return (s.same(ref, p.xp), s.same(ref, p.xm))

    own_kv.wait()
    down = s.start(kv.at[0, x], kv.at[1, x], p.nextrow)
    side = {0: both(kv.at[0, x])}
    own_w.wait()
    w_side = both(wout.at[yl, z, x])
    attend(0, x, diagonal=True)

    w_y = []
    far = {}

    def w_up(zz):
        w_y.append(s.same(wout.at[yl, zz], p.yf))

    def take_down(d):
        nonlocal down
        down.wait_recv()
        if d < 4:
            down = s.start(kv.at[d, x], kv.at[d + 1, x], p.nextrow)
        side[d] = both(kv.at[d, x])

    def take_side(d):
        side[d][0].wait_recv()
        one = s.same(kv.at[d, p.xs[3], pl.ds(0, 64)], p.xp)
        side[d][1].wait_recv()
        far[d] = (one, s.same(kv.at[d, p.xs[1], pl.ds(64, 64)], p.xm))

    def take_far(d):
        far[d][0].wait_recv()
        far[d][1].wait_recv()

    def w_forward(step):
        nonlocal w_z
        w_z[0].wait_recv()
        w_z[1].wait_recv()
        low, high_ = p.zs[NZ - step], p.zs[step]
        if step < 3:
            w_z = (s.same(wout.at[yl, low], p.zp), s.same(wout.at[yl, high_], p.zm))
        else:
            w_z = (
                s.same(wout.at[yl, low, pl.ds(0, 2)], p.zp),
                s.same(wout.at[yl, high_, pl.ds(2, 2)], p.zm),
            )
        w_up(low)
        w_up(high_)

    take_down(1)
    attend(1, x)
    take_side(0)
    w_side[0].wait_recv()
    w_far0 = s.same(wout.at[yl, z, p.xs[3], :, pl.ds(0, 2048)], p.xp)
    w_side[1].wait_recv()
    w_far1 = s.same(wout.at[yl, z, p.xs[1], :, pl.ds(2048, 2048)], p.xm)
    take_down(2)
    attend(2, x)
    w_far0.wait_recv()
    w_far1.wait_recv()
    w_z = (s.same(wout.at[yl, z], p.zp), s.same(wout.at[yl, z], p.zm))
    w_up(z)
    take_side(1)
    attend(1, p.xs[3])
    take_down(3)
    attend(1, p.xs[1])
    attend(3, x)
    take_side(2)
    w_forward(1)
    attend(2, p.xs[3])
    take_far(1)
    attend(1, p.xs[2])
    take_down(4)
    attend(2, p.xs[1])
    take_far(2)
    attend(2, p.xs[2])
    w_forward(2)
    take_side(3)
    attend(4, x)
    attend(3, p.xs[3])
    attend(3, p.xs[1])
    w_forward(3)
    take_side(4)
    take_far(3)
    attend(3, p.xs[2])
    take_far(0)

    def edge(k):
        xx = p.xs[k]
        attend(4 * lax.div(xx - x + 3, 4), xx)

    edge(3)
    edge(1)
    w_z[0].wait_recv()
    w_z[1].wait_recv()
    w_up(p.zs[4])
    take_far(4)
    edge(2)

    for j in range(QH):
        for t in range(4):
            rows = slice(t * PIECE, (t + 1) * PIECE)
            mixed[rows, j * HEAD : (j + 1) * HEAD] = (
                acc[j, rows, :HEAD] / acc[j, rows, HEAD:]
            ).astype(BF16)
    for copy in w_y:
        copy.wait_recv()
    out = pltpu.make_async_copy(wout, wout_out, copy_sem.at[2])
    out.start()
    s.drain()
    out.wait()


def attend_all(q, kv, start, wout):
    vmem = pl.BlockSpec(memory_space=pltpu.VMEM)
    hbm = pl.BlockSpec(memory_space=pl.ANY)
    return pl.pallas_call(
        attend_kernel,
        out_shape=(
            jax.ShapeDtypeStruct((BLK, QH * HEAD), BF16),
            jax.ShapeDtypeStruct((NYL, NZ, NX, 8, WIDTH), BF16),
        ),
        in_specs=[vmem, hbm, vmem, hbm],
        out_specs=(vmem, hbm),
        scratch_shapes=[
            pltpu.VMEM((5, NX, HEAD, 2 * BLK), BF16),
            pltpu.VMEM((NYL, NZ, NX, 8, WIDTH), BF16),
            pltpu.VMEM((QH, BLK, 2 * HEAD), F32),
            pltpu.VMEM((QH, BLK, HEAD), F32),
            pltpu.SemaphoreType.DMA((3,)),
            pltpu.SemaphoreType.DMA((64,)),
            pltpu.SemaphoreType.DMA((64,)),
        ],
        compiler_params=pltpu.CompilerParams(
            collective_id=2, has_side_effects=True, vmem_limit_bytes=48 << 20
        ),
        name="attend",
    )(q, kv, start, wout)


def on_device(tokens, w_query, key_value_weight, w_out, doc_lengths):
    blk_index = lax.axis_index("blk")
    positions = blk_index * BLK + jnp.arange(BLK, dtype=jnp.int32)
    ends = jnp.cumsum(doc_lengths)
    after = positions[:, None] >= ends[None, :]
    starts = jnp.sum(jnp.where(after, doc_lengths[None, :], 0), axis=1).astype(jnp.int32)
    half = HEAD // 2
    freqs = jnp.power(rope_base, -2.0 * jnp.arange(half, dtype=F32) / HEAD)
    angle = (positions - starts).astype(F32)[:, None] * freqs[None, :]
    cosine, sine = jnp.cos(angle), jnp.sin(angle)
    cos2 = jnp.concatenate([cosine, cosine], axis=1)
    sin2 = jnp.concatenate([-sine, sine], axis=1)
    start_rows = jnp.broadcast_to(starts[:, None], (BLK, HEAD))
    q, kv = project(tokens, w_query, key_value_weight.reshape(64, 256), cos2, sin2)
    mixed, head_rows = attend_all(q, kv, start_rows, w_out)
    return lax.psum_scatter(
        jnp.dot(
            mixed, head_rows.reshape(512, WIDTH), preferred_element_type=F32
        ).astype(BF16),
        "heads",
        scatter_dimension=0,
        tiled=True,
    )


def solution(mesh):
    return jax.shard_map(
        on_device,
        mesh=mesh,
        in_specs=(
            P(("blk", "heads"), None),
            P("blk", "heads"),
            P("blk", None, "heads"),
            P(("heads", "blk"), None),
            P(),
        ),
        out_specs=P(("blk", "heads"), None),
        check_vma=False,
    )
```

```python
import functools

import jax
import jax.numpy as jnp
from jax import lax
from jax.experimental import pallas as pl
from jax.experimental.pallas import tpu as pltpu
from jax.sharding import PartitionSpec as P

MESH = pl.DeviceIdType.MESH
BF16 = jnp.bfloat16
F32 = jnp.float32

HEAD = 128
QH = 4
BLK = 512
PIECE = 128
WIDTH = 4096
NX, NZ, NYL = 4, 8, 2
norm_epsilon = 1e-05
rope_base = 500000.0
masked_score = -1e30
LOG2E = 1.4426950408889634


class Place:
    def __init__(self):
        h = lax.axis_index("heads")
        b = lax.axis_index("blk")
        self.h, self.b = h, b
        self.yh, self.c = lax.div(h, 2), lax.rem(h, 2)
        self.yl = lax.div(b, NX * NZ)
        self.z = lax.rem(lax.div(b, NX), NZ)
        self.x = lax.rem(b, NX)
        self.row = b - self.x
        self.xs = [lax.rem(self.x + k, NX) for k in range(NX)]
        self.zs = [lax.rem(self.z + k, NZ) for k in range(NZ)]
        self.xp = (h, self.row + self.xs[1])
        self.xm = (h, self.row + self.xs[3])
        base = b - self.z * NX
        self.zp = (h, base + self.zs[1] * NX)
        self.zm = (h, base + self.zs[7] * NX)
        self.yf = (h, lax.rem(b + NX * NZ, 2 * NX * NZ))
        self.core = (h + 1 - 2 * self.c, b)
        y = 2 * self.yh + self.yl
        inner = lax.rem(b, NX * NZ)
        self.yp = self.at_y(lax.rem(y + 1, 4), inner)
        self.ym = self.at_y(lax.rem(y + 3, 4), inner)
        self.far = lax.rem(h + 2, 4)
        self.nextrow = (h, lax.rem(b + NX, 64))
        self.prevrow = (h, lax.rem(b + 60, 64))

    def at_y(self, y, inner):
        return (2 * lax.div(y, 2) + self.c, NX * NZ * lax.rem(y, 2) + inner)


def meet(devices):
    barrier = pltpu.get_barrier_semaphore()
    for device in devices:
        pl.semaphore_signal(barrier, inc=1, device_id=device, device_id_type=MESH)
    pl.semaphore_wait(barrier, len(devices))


class Sends:
    def __init__(self, send_sem, recv_sem):
        self.send_sem, self.recv_sem, self.made = send_sem, recv_sem, []

    def start(self, src, dst, device):
        i = len(self.made)
        copy = pltpu.make_async_remote_copy(
            src_ref=src,
            dst_ref=dst,
            send_sem=self.send_sem.at[i],
            recv_sem=self.recv_sem.at[i],
            device_id=device,
            device_id_type=MESH,
        )
        copy.start()
        self.made.append(copy)
        return copy

    def same(self, ref, device):
        return self.start(ref, ref, device)

    def drain(self):
        for copy in self.made:
            copy.wait_send()


def project_kernel(
    tokens, wq_in, wkv_in, cos, sin, q_out, kv_out,
    xbuf, ra, rb, wq, wkv, acc, copy_sem, send_sem, recv_sem,
):
    p = Place()
    x, z, yl, h = p.x, p.z, p.yl, p.h
    own_q = pltpu.make_async_copy(wq_in, wq.at[yl, z, x], copy_sem.at[0])
    own_kv = pltpu.make_async_copy(wkv_in, wkv.at[yl, z, x], copy_sem.at[1])
    own_q.start()
    own_kv.start()
    meet([p.xp, p.xm, p.zp, p.zm, p.yp, p.ym, p.core])
    s = Sends(send_sem, recv_sem)
    own_kv.wait()
    y_kv = s.same(wkv.at[yl, z, x], p.yf)
    own_q.wait()
    y_q = s.same(wq.at[yl, z, x], p.yf)

    def normalize(i, carry):
        rows = pl.ds(pl.multiple_of(i * 16, 16), 16)
        v = tokens[rows, :].astype(F32)
        mean = jnp.mean(v * v, axis=1, keepdims=True)
        xbuf[h, rows, :] = (v * lax.rsqrt(mean + norm_epsilon)).astype(BF16)
        return carry

    lax.fori_loop(0, PIECE // 16, normalize, 0)

    y_kv.wait_recv()
    ax = (s.same(wkv.at[:, z, x], p.xp), s.same(wkv.at[:, z, x], p.xm))
    y_q.wait_recv()
    bz = (s.same(wq.at[:, z, x], p.zp), s.same(wq.at[:, z, x], p.zm))

    def bx_send(zz):
        return (s.same(wq.at[:, zz, x], p.xp), s.same(wq.at[:, zz, x], p.xm))

    def bx_forward(zz, pair):
        pair[0].wait_recv()
        one = s.same(wq.at[0, zz, p.xs[3]], p.xp)
        pair[1].wait_recv()
        return (one, s.same(wq.at[1, zz, p.xs[1]], p.xm))

    rows0 = bx_send(z)
    act_core = s.same(xbuf.at[h], p.core)
    act = (
        s.start(xbuf.at[h, pl.ds(0, 64)], ra, p.yp),
        s.start(xbuf.at[h, pl.ds(64, 64)], rb, p.ym),
    )

    def z_forward(buf, pair, step, pick):
        pair[0].wait_recv()
        pair[1].wait_recv()
        low, high = p.zs[NZ - step], p.zs[step]
        if step < NZ // 2 - 1:
            return (s.same(pick(buf, None, low), p.zp), s.same(pick(buf, None, high), p.zm))
        return (s.same(pick(buf, 0, low), p.zp), s.same(pick(buf, 1, high), p.zm))

    def pick_b(buf, part, zz):
        return buf.at[:, zz, x] if part is None else buf.at[part, zz, x]

    def pick_a(buf, part, zz):
        return buf.at[:, zz] if part is None else buf.at[part, zz]

    ax[0].wait_recv()
    ax_far0 = s.same(wkv.at[0, z, p.xs[3]], p.xp)
    ax[1].wait_recv()
    ax_far1 = s.same(wkv.at[1, z, p.xs[1]], p.xm)
    bz = z_forward(wq, bz, 1, pick_b)
    rows1 = (bx_send(p.zs[7]), bx_send(p.zs[1]))
    ax_far0.wait_recv()
    ax_far1.wait_recv()
    bz = z_forward(wq, bz, 2, pick_b)
    az = (s.same(pick_a(wkv, None, z), p.zp), s.same(pick_a(wkv, None, z), p.zm))
    rows2 = (bx_send(p.zs[6]), bx_send(p.zs[2]))
    far0 = bx_forward(z, rows0)
    act[0].wait_recv()
    hm = p.ym[0]
    hp = p.yp[0]
    relay0 = s.start(ra, xbuf.at[hm, pl.ds(0, 64)], p.yp)
    act[1].wait_recv()
    relay1 = s.start(rb, xbuf.at[hp, pl.ds(64, 64)], p.ym)
    bz = z_forward(wq, bz, 3, pick_b)
    rows3 = (bx_send(p.zs[5]), bx_send(p.zs[3]))
    far1 = (bx_forward(p.zs[7], rows1[0]), bx_forward(p.zs[1], rows1[1]))
    az = z_forward(wkv, az, 1, pick_a)
    bz[0].wait_recv()
    bz[1].wait_recv()
    rows4 = bx_send(p.zs[4])
    az = z_forward(wkv, az, 2, pick_a)
    far2 = (bx_forward(p.zs[6], rows2[0]), bx_forward(p.zs[2], rows2[1]))
    relay0.wait_recv()
    relay1.wait_recv()
    act_far = s.same(xbuf.at[p.far], p.core)
    az = z_forward(wkv, az, 3, pick_a)
    far3 = (bx_forward(p.zs[5], rows3[0]), bx_forward(p.zs[3], rows3[1]))
    far4 = bx_forward(p.zs[4], rows4)
    for pair in (az, far0, far1[0], far1[1], far2[0], far2[1], far3[0], far3[1], far4):
        pair[0].wait_recv()
        pair[1].wait_recv()
    act_core.wait_recv()
    act_far.wait_recv()

    def multiply(k, carry):
        left = xbuf[:, :, pl.ds(pl.multiple_of(k * 512, 512), 512)].reshape(BLK, 512)
        ky = lax.div(k, 4)
        kz = 2 * lax.rem(k, 4)
        right = wq[ky, pl.ds(kz, 2)].reshape(512, 512)
        acc[:, :512] += jnp.dot(left, right, preferred_element_type=F32)
        right = wkv[ky, pl.ds(kz, 2)].reshape(512, 256)
        acc[:, 512:] += jnp.dot(left, right, preferred_element_type=F32)
        return carry

    acc[...] = jnp.zeros_like(acc)
    lax.fori_loop(0, 8, multiply, 0)

    for t in range(4):
        rows = slice(t * PIECE, (t + 1) * PIECE)
        co, si = cos[rows, :], sin[rows, :]

        def rotated(at):
            v = acc[rows, at : at + HEAD]
            return v * co + pltpu.roll(v, HEAD // 2, 1) * si

        for j in range(QH):
            q_out[j, rows, :] = rotated(j * HEAD).astype(BF16)
        kv_out[:, rows] = rotated(QH * HEAD).T.astype(BF16)
        kv_out[:, BLK + t * PIECE : BLK + (t + 1) * PIECE] = acc[rows, 640:768].astype(BF16)
    s.drain()


def project(tokens, wq, wkv, cos, sin):
    vmem = pl.BlockSpec(memory_space=pltpu.VMEM)
    hbm = pl.BlockSpec(memory_space=pl.ANY)
    return pl.pallas_call(
        project_kernel,
        out_shape=(
            jax.ShapeDtypeStruct((QH, BLK, HEAD), BF16),
            jax.ShapeDtypeStruct((HEAD, 2 * BLK), BF16),
        ),
        in_specs=[vmem, hbm, hbm, vmem, vmem],
        out_specs=(vmem, vmem),
        scratch_shapes=[
            pltpu.VMEM((4, PIECE, WIDTH), BF16),
            pltpu.VMEM((64, WIDTH), BF16),
            pltpu.VMEM((64, WIDTH), BF16),
            pltpu.VMEM((NYL, NZ, NX, 64, 512), BF16),
            pltpu.VMEM((NYL, NZ, NX, 64, 256), BF16),
            pltpu.VMEM((BLK, 768), F32),
            pltpu.SemaphoreType.DMA((2,)),
            pltpu.SemaphoreType.DMA((64,)),
            pltpu.SemaphoreType.DMA((64,)),
        ],
        compiler_params=pltpu.CompilerParams(
            collective_id=1, has_side_effects=True, vmem_limit_bytes=48 << 20
        ),
        name="project",
    )(tokens, wq, wkv, cos, sin)


def attend_kernel(
    q, kv_in, start, wout_in, mixed, wout,
    kv, acc, high, copy_sem, send_sem, recv_sem,
):
    p = Place()
    x, z, yl = p.x, p.z, p.yl
    own_kv = pltpu.make_async_copy(kv_in, kv.at[0, x], copy_sem.at[0])
    own_w = pltpu.make_async_copy(wout_in, wout.at[yl, z, x], copy_sem.at[1])
    own_kv.start()
    own_w.start()
    meet([p.xp, p.xm, p.zp, p.zm, p.yf, p.nextrow, p.prevrow])
    s = Sends(send_sem, recv_sem)
    factor = HEAD ** (-0.5) * LOG2E
    lane = lax.broadcasted_iota(jnp.int32, (256, BLK), 1)

    def attend(d, xx, diagonal=False):
        base = p.row * BLK + (xx - NX * d) * BLK
        keys = kv[d, xx, :, 0:BLK]
        vals = jnp.concatenate(
            [kv[d, xx, :, BLK + i * HEAD : BLK + (i + 1) * HEAD] for i in range(4)], axis=0
        )
        vals = jnp.concatenate([vals, jnp.ones((BLK, HEAD), BF16)], axis=1)

        def head(j, carry):
            for half in range(2):
                rows = slice(half * 256, half * 256 + 256)
                score = jnp.dot(q[j, rows, :], keys, preferred_element_type=F32) * factor
                first = start[rows, :] - base
                keep = lane >= jnp.concatenate([first] * 4, axis=1)
                if diagonal:
                    keep &= lane <= lax.broadcasted_iota(jnp.int32, (256, BLK), 0) + half * 256
                score = jnp.where(keep, score, masked_score)
                top = jnp.max(score, axis=1, keepdims=True)
                if diagonal:
                    new = jnp.broadcast_to(top, (256, HEAD))
                else:
                    old = high[j, rows, :]
                    new = jnp.maximum(old, top)
                probs = jnp.exp2(score - jnp.concatenate([new] * 4, axis=1)).astype(BF16)
                update = jnp.dot(probs, vals, preferred_element_type=F32)
                if not diagonal:
                    fade = jnp.exp2(old - new)
                    update += acc[j, rows, :] * jnp.concatenate([fade, fade], axis=1)
                acc[j, rows, :] = update
                high[j, rows, :] = new
            return carry

        lax.fori_loop(0, QH, head, 0)

    def both(ref):
        return (s.same(ref, p.xp), s.same(ref, p.xm))

    own_kv.wait()
    down = s.start(kv.at[0, x], kv.at[1, x], p.nextrow)
    side = {0: both(kv.at[0, x])}
    own_w.wait()
    w_side = both(wout.at[yl, z, x])
    attend(0, x, diagonal=True)

    w_y = []
    far = {}

    def w_up(zz):
        w_y.append(s.same(wout.at[yl, zz], p.yf))

    def take_down(d):
        nonlocal down
        down.wait_recv()
        if d < 4:
            down = s.start(kv.at[d, x], kv.at[d + 1, x], p.nextrow)
        side[d] = both(kv.at[d, x])

    def take_side(d):
        side[d][0].wait_recv()
        one = s.same(kv.at[d, p.xs[3], pl.ds(0, 64)], p.xp)
        side[d][1].wait_recv()
        far[d] = (one, s.same(kv.at[d, p.xs[1], pl.ds(64, 64)], p.xm))

    def take_far(d):
        far[d][0].wait_recv()
        far[d][1].wait_recv()

    def w_forward(step):
        nonlocal w_z
        w_z[0].wait_recv()
        w_z[1].wait_recv()
        low, high_ = p.zs[NZ - step], p.zs[step]
        if step < 3:
            w_z = (s.same(wout.at[yl, low], p.zp), s.same(wout.at[yl, high_], p.zm))
        else:
            w_z = (
                s.same(wout.at[yl, low, pl.ds(0, 2)], p.zp),
                s.same(wout.at[yl, high_, pl.ds(2, 2)], p.zm),
            )
        w_up(low)
        w_up(high_)

    take_down(1)
    attend(1, x)
    take_side(0)
    w_side[0].wait_recv()
    w_far0 = s.same(wout.at[yl, z, p.xs[3], :, pl.ds(0, 2048)], p.xp)
    w_side[1].wait_recv()
    w_far1 = s.same(wout.at[yl, z, p.xs[1], :, pl.ds(2048, 2048)], p.xm)
    take_down(2)
    attend(2, x)
    w_far0.wait_recv()
    w_far1.wait_recv()
    w_z = (s.same(wout.at[yl, z], p.zp), s.same(wout.at[yl, z], p.zm))
    w_up(z)
    take_side(1)
    attend(1, p.xs[3])
    take_down(3)
    attend(1, p.xs[1])
    attend(3, x)
    take_side(2)
    w_forward(1)
    attend(2, p.xs[3])
    take_far(1)
    attend(1, p.xs[2])
    take_down(4)
    attend(2, p.xs[1])
    take_far(2)
    attend(2, p.xs[2])
    w_forward(2)
    take_side(3)
    attend(4, x)
    attend(3, p.xs[3])
    attend(3, p.xs[1])
    w_forward(3)
    take_side(4)
    take_far(3)
    attend(3, p.xs[2])
    take_far(0)

    def edge(k):
        xx = p.xs[k]
        attend(4 * lax.div(xx - x + 3, 4), xx)

    edge(3)
    edge(1)
    w_z[0].wait_recv()
    w_z[1].wait_recv()
    w_up(p.zs[4])
    take_far(4)
    edge(2)

    for j in range(QH):
        for t in range(4):
            rows = slice(t * PIECE, (t + 1) * PIECE)
            mixed[rows, j * HEAD : (j + 1) * HEAD] = (
                acc[j, rows, :HEAD] / acc[j, rows, HEAD:]
            ).astype(BF16)
    for copy in w_y:
        copy.wait_recv()
    s.drain()


def attend_all(q, kv, start, wout):
    vmem = pl.BlockSpec(memory_space=pltpu.VMEM)
    hbm = pl.BlockSpec(memory_space=pl.ANY)
    return pl.pallas_call(
        attend_kernel,
        out_shape=(
            jax.ShapeDtypeStruct((BLK, QH * HEAD), BF16),
            jax.ShapeDtypeStruct((NYL, NZ, NX, 8, WIDTH), BF16),
        ),
        in_specs=[vmem, hbm, vmem, hbm],
        out_specs=(vmem, vmem),
        scratch_shapes=[
            pltpu.VMEM((5, NX, HEAD, 2 * BLK), BF16),
            pltpu.VMEM((QH, BLK, 2 * HEAD), F32),
            pltpu.VMEM((QH, BLK, HEAD), F32),
            pltpu.SemaphoreType.DMA((2,)),
            pltpu.SemaphoreType.DMA((64,)),
            pltpu.SemaphoreType.DMA((64,)),
        ],
        compiler_params=pltpu.CompilerParams(
            collective_id=2, has_side_effects=True, vmem_limit_bytes=48 << 20
        ),
        name="attend",
    )(q, kv, start, wout)


NCHUNK, CHUNK = 8, 512


def output_kernel(
    mixed, w, out, give_far, take_far, own_far, sum_far, via, got, give_near, take_near, own,
    send_sem, recv_sem,
):
    p = Place()
    other = p.h + 1 - 2 * p.c
    far_other = lax.rem(other + 2, 4)
    meet([p.yp, p.ym, p.core])
    s = Sends(send_sem, recv_sem)

    def times(owner, n):
        rows = pl.ds(pl.multiple_of(owner * PIECE, PIECE), PIECE)
        return jnp.dot(
            mixed[rows, :], w[:, n * CHUNK : (n + 1) * CHUNK], preferred_element_type=F32
        )

    def toward(n):
        return p.yp if n % 2 == 0 else p.ym

    to_core, hops, near = [], [], []

    def combine(n):
        to_core[n].wait_recv()
        sum_far[n] = (own_far[n] + take_far[n].astype(F32)).astype(BF16)
        hops.append(s.start(sum_far.at[n], via.at[n], toward(n)))

    for n in range(NCHUNK):
        give_far[n] = times(far_other, n).astype(BF16)
        to_core.append(s.start(give_far.at[n], take_far.at[n], p.core))
        own_far[n] = times(p.far, n)
        if n >= 2:
            combine(n - 2)
    combine(NCHUNK - 2)
    combine(NCHUNK - 1)
    for n in range(NCHUNK):
        give_near[n] = times(other, n).astype(BF16)
        near.append(s.start(give_near.at[n], take_near.at[n], p.core))
        own[n] = times(p.h, n)
    last = []
    for n in range(NCHUNK):
        hops[n].wait_recv()
        last.append(s.start(via.at[n], got.at[n], toward(n)))
    for n in range(NCHUNK):
        near[n].wait_recv()
        own[n] += take_near[n].astype(F32)
    for n in range(NCHUNK):
        last[n].wait_recv()
        out[:, n * CHUNK : (n + 1) * CHUNK] = (own[n] + got[n].astype(F32)).astype(BF16)
    s.drain()


def project_out(mixed, w):
    vmem = pl.BlockSpec(memory_space=pltpu.VMEM)
    piece = pltpu.VMEM((NCHUNK, PIECE, CHUNK), BF16)
    wide = pltpu.VMEM((NCHUNK, PIECE, CHUNK), F32)
    return pl.pallas_call(
        output_kernel,
        out_shape=jax.ShapeDtypeStruct((PIECE, WIDTH), BF16),
        in_specs=[vmem, vmem],
        out_specs=vmem,
        scratch_shapes=[
            piece, piece, wide, piece, piece, piece, piece, piece, wide,
            pltpu.SemaphoreType.DMA((32,)),
            pltpu.SemaphoreType.DMA((32,)),
        ],
        compiler_params=pltpu.CompilerParams(
            collective_id=3, has_side_effects=True, vmem_limit_bytes=48 << 20
        ),
        name="output",
    )(mixed, w)


def on_device(tokens, w_query, key_value_weight, w_out, doc_lengths):
    blk_index = lax.axis_index("blk")
    positions = blk_index * BLK + jnp.arange(BLK, dtype=jnp.int32)
    ends = jnp.cumsum(doc_lengths)
    after = positions[:, None] >= ends[None, :]
    starts = jnp.sum(jnp.where(after, doc_lengths[None, :], 0), axis=1).astype(jnp.int32)
    half = HEAD // 2
    freqs = jnp.power(rope_base, -2.0 * jnp.arange(half, dtype=F32) / HEAD)
    angle = (positions - starts).astype(F32)[:, None] * freqs[None, :]
    cosine, sine = jnp.cos(angle), jnp.sin(angle)
    cos2 = jnp.concatenate([cosine, cosine], axis=1)
    sin2 = jnp.concatenate([-sine, sine], axis=1)
    start_rows = jnp.broadcast_to(starts[:, None], (BLK, HEAD))
    q, kv = project(tokens, w_query, key_value_weight.reshape(64, 256), cos2, sin2)
    mixed, head_rows = attend_all(q, kv, start_rows, w_out)
    return project_out(mixed, head_rows.reshape(512, WIDTH))


def solution(mesh):
    return jax.shard_map(
        on_device,
        mesh=mesh,
        in_specs=(
            P(("blk", "heads"), None),
            P("blk", "heads"),
            P("blk", None, "heads"),
            P(("heads", "blk"), None),
            P(),
        ),
        out_specs=P(("blk", "heads"), None),
        check_vma=False,
    )
```

```python
import functools

import jax
import jax.numpy as jnp
from jax import lax
from jax.experimental import pallas as pl
from jax.experimental.pallas import tpu as pltpu
from jax.sharding import PartitionSpec as P

MESH = pl.DeviceIdType.MESH
BF16 = jnp.bfloat16
F32 = jnp.float32

HEAD = 128
QH = 4
BLK = 512
PIECE = 128
WIDTH = 4096
NX, NZ, NYL = 4, 8, 2
norm_epsilon = 1e-05
rope_base = 500000.0
masked_score = -1e30
LOG2E = 1.4426950408889634


class Place:
    def __init__(self):
        h = lax.axis_index("heads")
        b = lax.axis_index("blk")
        self.h, self.b = h, b
        self.yh, self.c = lax.div(h, 2), lax.rem(h, 2)
        self.yl = lax.div(b, NX * NZ)
        self.z = lax.rem(lax.div(b, NX), NZ)
        self.x = lax.rem(b, NX)
        self.row = b - self.x
        self.xs = [lax.rem(self.x + k, NX) for k in range(NX)]
        self.zs = [lax.rem(self.z + k, NZ) for k in range(NZ)]
        self.xp = (h, self.row + self.xs[1])
        self.xm = (h, self.row + self.xs[3])
        base = b - self.z * NX
        self.zp = (h, base + self.zs[1] * NX)
        self.zm = (h, base + self.zs[7] * NX)
        self.yf = (h, lax.rem(b + NX * NZ, 2 * NX * NZ))
        self.core = (h + 1 - 2 * self.c, b)
        y = 2 * self.yh + self.yl
        inner = lax.rem(b, NX * NZ)
        self.yp = self.at_y(lax.rem(y + 1, 4), inner)
        self.ym = self.at_y(lax.rem(y + 3, 4), inner)
        self.far = lax.rem(h + 2, 4)
        self.nextrow = (h, lax.rem(b + NX, 64))
        self.prevrow = (h, lax.rem(b + 60, 64))

    def at_y(self, y, inner):
        return (2 * lax.div(y, 2) + self.c, NX * NZ * lax.rem(y, 2) + inner)


def meet(devices):
    barrier = pltpu.get_barrier_semaphore()
    for device in devices:
        pl.semaphore_signal(barrier, inc=1, device_id=device, device_id_type=MESH)
    pl.semaphore_wait(barrier, len(devices))


class Sends:
    def __init__(self, send_sem, recv_sem):
        self.send_sem, self.recv_sem, self.made = send_sem, recv_sem, []

    def start(self, src, dst, device):
        i = len(self.made)
        copy = pltpu.make_async_remote_copy(
            src_ref=src,
            dst_ref=dst,
            send_sem=self.send_sem.at[i],
            recv_sem=self.recv_sem.at[i],
            device_id=device,
            device_id_type=MESH,
        )
        copy.start()
        self.made.append(copy)
        return copy

    def same(self, ref, device):
        return self.start(ref, ref, device)

    def drain(self):
        for copy in self.made:
            copy.wait_send()


FACTOR = HEAD ** (-0.5) * LOG2E


def attention_kernel(
    tokens_in, wq_in, wkv_in, wout_in, cos, sin, start, mixed, wout,
    tokens, xbuf, ra, rb, wq, wkv, raw, qt, kv, acc, high, copy_sem, send_sem, recv_sem,
):
    p = Place()
    x, z, yl, h = p.x, p.z, p.yl, p.h
    own = [
        pltpu.make_async_copy(wkv_in, wkv.at[yl, z, x], copy_sem.at[0]),
        pltpu.make_async_copy(wq_in, wq.at[yl, z, x], copy_sem.at[1]),
        pltpu.make_async_copy(tokens_in, tokens, copy_sem.at[2]),
        pltpu.make_async_copy(wout_in, wout.at[yl, z, x], copy_sem.at[3]),
    ]
    for copy in own:
        copy.start()
    meet([p.xp, p.xm, p.zp, p.zm, p.yp, p.ym, p.core, p.nextrow, p.prevrow])
    s = Sends(send_sem, recv_sem)

    def both(ref):
        return (s.same(ref, p.xp), s.same(ref, p.xm))

    def settle(pair):
        pair[0].wait_recv()
        pair[1].wait_recv()

    own[0].wait()
    y_kv = s.same(wkv.at[yl, z, x], p.yf)
    own[1].wait()
    y_q = s.same(wq.at[yl, z, x], p.yf)
    own[2].wait()

    def normalize(i, carry):
        rows = pl.ds(pl.multiple_of(i * 16, 16), 16)
        v = tokens[rows, :].astype(F32)
        mean = jnp.mean(v * v, axis=1, keepdims=True)
        xbuf[h, rows, :] = (v * lax.rsqrt(mean + norm_epsilon)).astype(BF16)
        return carry

    lax.fori_loop(0, PIECE // 16, normalize, 0)

    def bx_send(zz):
        return both(wq.at[:, zz, x])

    def bx_forward(zz, pair):
        pair[0].wait_recv()
        one = s.same(wq.at[0, zz, p.xs[3]], p.xp)
        pair[1].wait_recv()
        return (one, s.same(wq.at[1, zz, p.xs[1]], p.xm))

    def z_forward(pair, step, pick):
        settle(pair)
        low, high_ = p.zs[NZ - step], p.zs[step]
        if step < NZ // 2 - 1:
            return (s.same(pick(None, low), p.zp), s.same(pick(None, high_), p.zm))
        return (s.same(pick(0, low), p.zp), s.same(pick(1, high_), p.zm))

    def pick_b(part, zz):
        return wq.at[:, zz, x] if part is None else wq.at[part, zz, x]

    def pick_a(part, zz):
        return wkv.at[:, zz] if part is None else wkv.at[part, zz]

    def pick_w(part, zz):
        return wout.at[yl, zz] if part is None else wout.at[yl, zz, pl.ds(2 * part, 2)]

    y_kv.wait_recv()
    ax = both(wkv.at[:, z, x])
    y_q.wait_recv()
    bz = (s.same(wq.at[:, z, x], p.zp), s.same(wq.at[:, z, x], p.zm))
    rows0 = bx_send(z)
    act_core = s.same(xbuf.at[h], p.core)
    act = (
        s.start(xbuf.at[h, pl.ds(0, 64)], ra, p.yp),
        s.start(xbuf.at[h, pl.ds(64, 64)], rb, p.ym),
    )
    ax[0].wait_recv()
    ax_far0 = s.same(wkv.at[0, z, p.xs[3]], p.xp)
    ax[1].wait_recv()
    ax_far = (ax_far0, s.same(wkv.at[1, z, p.xs[1]], p.xm))
    bz = z_forward(bz, 1, pick_b)
    rows1 = (bx_send(p.zs[7]), bx_send(p.zs[1]))
    settle(ax_far)
    az = (s.same(pick_a(None, z), p.zp), s.same(pick_a(None, z), p.zm))
    bz = z_forward(bz, 2, pick_b)
    rows2 = (bx_send(p.zs[6]), bx_send(p.zs[2]))
    far0 = bx_forward(z, rows0)
    own[3].wait()
    w_side = both(wout.at[yl, z, x])
    act[0].wait_recv()
    relay0 = s.start(ra, xbuf.at[p.ym[0], pl.ds(0, 64)], p.yp)
    act[1].wait_recv()
    relay1 = s.start(rb, xbuf.at[p.yp[0], pl.ds(64, 64)], p.ym)
    az = z_forward(az, 1, pick_a)
    bz = z_forward(bz, 3, pick_b)
    rows3 = (bx_send(p.zs[5]), bx_send(p.zs[3]))
    far1 = (bx_forward(p.zs[7], rows1[0]), bx_forward(p.zs[1], rows1[1]))
    w_side[0].wait_recv()
    w_far0 = s.same(wout.at[yl, z, p.xs[3], :, pl.ds(0, 2048)], p.xp)
    w_side[1].wait_recv()
    w_far = (w_far0, s.same(wout.at[yl, z, p.xs[1], :, pl.ds(2048, 2048)], p.xm))
    az = z_forward(az, 2, pick_a)
    settle(bz)
    rows4 = bx_send(p.zs[4])
    far2 = (bx_forward(p.zs[6], rows2[0]), bx_forward(p.zs[2], rows2[1]))
    settle((relay0, relay1))
    act_far = s.same(xbuf.at[p.far], p.core)
    az = z_forward(az, 3, pick_a)
    settle(w_far)
    w_y = []

    def w_up(zz):
        w_y.append(s.same(wout.at[yl, zz], p.yf))

    w_z = (s.same(pick_w(None, z), p.zp), s.same(pick_w(None, z), p.zm))
    w_up(z)

    def w_forward(step):
        nonlocal w_z
        w_z = z_forward(w_z, step, pick_w)
        w_up(p.zs[NZ - step])
        w_up(p.zs[step])

    far3 = (bx_forward(p.zs[5], rows3[0]), bx_forward(p.zs[3], rows3[1]))
    settle(az)
    settle((act_core, act_far))

    def left_of(k):
        return xbuf[:, :, pl.ds(pl.multiple_of(k * 512, 512), 512)].reshape(BLK, 512)

    def multiply_kv(k, carry):
        right = wkv[lax.div(k, 4), pl.ds(2 * lax.rem(k, 4), 2)].reshape(512, 256)
        raw[:, 512:] += jnp.dot(left_of(k), right, preferred_element_type=F32)
        return carry

    def multiply_q(k, carry):
        right = wq[lax.div(k, 4), pl.ds(2 * lax.rem(k, 4), 2)].reshape(512, 512)
        raw[:, :512] += jnp.dot(left_of(k), right, preferred_element_type=F32)
        return carry

    def rotated(rows, at):
        v = raw[rows, at : at + HEAD]
        return v * cos[rows, :] + pltpu.roll(v, HEAD // 2, 1) * sin[rows, :]

    raw[...] = jnp.zeros_like(raw)
    lax.fori_loop(0, 8, multiply_kv, 0)
    for t in range(4):
        rows = slice(t * PIECE, (t + 1) * PIECE)
        kv[0, x, :, rows] = raw[rows, 640:768].T.astype(BF16)
        kv[0, x, :, BLK + t * PIECE : BLK + (t + 1) * PIECE] = rotated(rows, 512).astype(BF16)
    far4 = bx_forward(p.zs[4], rows4)
    down = s.start(kv.at[0, x], kv.at[1, x], p.nextrow)
    side = {0: both(kv.at[0, x])}
    far = {}

    for pair in (far0, far1[0], far1[1], far2[0], far2[1], far3[0], far3[1], far4):
        settle(pair)
    lax.fori_loop(0, 8, multiply_q, 0)
    for j in range(QH):
        for t in range(4):
            rows = slice(t * PIECE, (t + 1) * PIECE)
            qt[:, j * BLK + t * PIECE : j * BLK + (t + 1) * PIECE] = (
                (rotated(rows, j * HEAD) * FACTOR).T.astype(BF16)
            )

    key_at = lax.broadcasted_iota(jnp.int32, (BLK, BLK), 0)

    def attend(d, xx, diagonal=False):
        first = start[...] - (p.row + xx - NX * d) * BLK
        keys = jnp.concatenate(
            [kv[d, xx, :, BLK + i * HEAD : BLK + (i + 1) * HEAD] for i in range(4)], axis=0
        )
        vals = jnp.concatenate([kv[d, xx, :, :BLK], jnp.ones((16, BLK), BF16)], axis=0)

        def scores(j):
            return jnp.dot(
                keys, qt[:, j * BLK : (j + 1) * BLK], preferred_element_type=F32
            )

        def finish(j, score):
            at = slice(j * BLK, (j + 1) * BLK)
            keep = key_at >= first
            if diagonal:
                keep &= key_at <= lax.broadcasted_iota(jnp.int32, (BLK, BLK), 1)
            score = jnp.where(keep, score, masked_score)
            new = jnp.max(score, axis=0, keepdims=True)
            if not diagonal:
                old = high[:, at]
                new = jnp.maximum(old, new)
            probs = jnp.exp2(score - new).astype(BF16)
            update = jnp.dot(vals, probs, preferred_element_type=F32)
            if not diagonal:
                update += acc[:, at] * jnp.exp2(old - new)
            acc[:, at] = update
            high[:, at] = new

        now = scores(0)
        for j in range(QH):
            later = scores(j + 1) if j + 1 < QH else None
            finish(j, now)
            now = later

    def take_down(d):
        nonlocal down
        down.wait_recv()
        if d < 4:
            down = s.start(kv.at[d, x], kv.at[d + 1, x], p.nextrow)
        side[d] = both(kv.at[d, x])

    def take_side(d):
        side[d][0].wait_recv()
        one = s.same(kv.at[d, p.xs[3], pl.ds(0, 64)], p.xp)
        side[d][1].wait_recv()
        far[d] = (one, s.same(kv.at[d, p.xs[1], pl.ds(64, 64)], p.xm))

    def take_far(d):
        settle(far[d])

    w_forward(1)
    attend(0, x, diagonal=True)
    take_down(1)
    take_side(0)
    attend(1, x)
    w_forward(2)
    take_down(2)
    attend(2, x)
    take_side(1)
    attend(1, p.xs[3])
    attend(1, p.xs[1])
    take_down(3)
    attend(3, x)
    w_forward(3)
    take_side(2)
    take_far(1)
    attend(1, p.xs[2])
    attend(2, p.xs[3])
    attend(2, p.xs[1])
    take_down(4)
    attend(4, x)
    take_side(3)
    take_far(2)
    attend(2, p.xs[2])
    settle(w_z)
    w_up(p.zs[4])
    attend(3, p.xs[3])
    attend(3, p.xs[1])
    take_side(4)
    take_far(3)
    attend(3, p.xs[2])
    take_far(0)

    def edge(k):
        xx = p.xs[k]
        attend(4 * lax.div(xx - x + 3, 4), xx)

    edge(3)
    edge(1)
    take_far(4)
    edge(2)

    for j in range(QH):
        for t in range(4):
            at = slice(j * BLK + t * PIECE, j * BLK + (t + 1) * PIECE)
            part = acc[:HEAD, at] * (1.0 / acc[HEAD : HEAD + 1, at])
            mixed[t * PIECE : (t + 1) * PIECE, j * HEAD : (j + 1) * HEAD] = part.T.astype(BF16)
    for copy in w_y:
        copy.wait_recv()
    s.drain()


def attention(tokens, wq, wkv, wout, cos, sin, start):
    vmem = pl.BlockSpec(memory_space=pltpu.VMEM)
    hbm = pl.BlockSpec(memory_space=pltpu.HBM)
    return pl.pallas_call(
        attention_kernel,
        out_shape=(
            jax.ShapeDtypeStruct((BLK, QH * HEAD), BF16),
            jax.ShapeDtypeStruct((NYL, NZ, NX, 8, WIDTH), BF16),
        ),
        in_specs=[hbm, hbm, hbm, hbm, vmem, vmem, vmem],
        out_specs=(vmem, vmem),
        scratch_shapes=[
            pltpu.VMEM((PIECE, WIDTH), BF16),
            pltpu.VMEM((4, PIECE, WIDTH), BF16),
            pltpu.VMEM((64, WIDTH), BF16),
            pltpu.VMEM((64, WIDTH), BF16),
            pltpu.VMEM((NYL, NZ, NX, 64, 512), BF16),
            pltpu.VMEM((NYL, NZ, NX, 64, 256), BF16),
            pltpu.VMEM((BLK, 768), F32),
            pltpu.VMEM((HEAD, QH * BLK), BF16),
            pltpu.VMEM((5, NX, HEAD, 2 * BLK), BF16),
            pltpu.VMEM((HEAD + 16, QH * BLK), F32),
            pltpu.VMEM((1, QH * BLK), F32),
            pltpu.SemaphoreType.DMA((4,)),
            pltpu.SemaphoreType.DMA((112,)),
            pltpu.SemaphoreType.DMA((112,)),
        ],
        compiler_params=pltpu.CompilerParams(
            collective_id=1, has_side_effects=True, vmem_limit_bytes=36 << 20
        ),
        name="attention",
    )(tokens, wq, wkv, wout, cos, sin, start)


NCHUNK, CHUNK = 8, 512


def output_kernel(
    mixed, w, out, give_far, take_far, own_far, sum_far, via, got, give_near, take_near, own,
    send_sem, recv_sem,
):
    p = Place()
    other = p.h + 1 - 2 * p.c
    far_other = lax.rem(other + 2, 4)
    meet([p.yp, p.ym, p.core])
    s = Sends(send_sem, recv_sem)

    def times(owner, n):
        rows = pl.ds(pl.multiple_of(owner * PIECE, PIECE), PIECE)
        return jnp.dot(
            mixed[rows, :], w[:, n * CHUNK : (n + 1) * CHUNK], preferred_element_type=F32
        )

    def toward(n):
        return p.yp if n % 2 == 0 else p.ym

    to_core, hops, near = [], [], []

    def combine(n):
        to_core[n].wait_recv()
        sum_far[n] = (own_far[n] + take_far[n].astype(F32)).astype(BF16)
        hops.append(s.start(sum_far.at[n], via.at[n], toward(n)))

    for n in range(NCHUNK):
        give_far[n] = times(far_other, n).astype(BF16)
        to_core.append(s.start(give_far.at[n], take_far.at[n], p.core))
        own_far[n] = times(p.far, n)
        if n >= 2:
            combine(n - 2)
    combine(NCHUNK - 2)
    combine(NCHUNK - 1)
    for n in range(NCHUNK):
        give_near[n] = times(other, n).astype(BF16)
        near.append(s.start(give_near.at[n], take_near.at[n], p.core))
        own[n] = times(p.h, n)
    last = []
    for n in range(NCHUNK):
        hops[n].wait_recv()
        last.append(s.start(via.at[n], got.at[n], toward(n)))
    for n in range(NCHUNK):
        near[n].wait_recv()
        own[n] += take_near[n].astype(F32)
    for n in range(NCHUNK):
        last[n].wait_recv()
        out[:, n * CHUNK : (n + 1) * CHUNK] = (own[n] + got[n].astype(F32)).astype(BF16)
    s.drain()


def project_out(mixed, w):
    vmem = pl.BlockSpec(memory_space=pltpu.VMEM)
    piece = pltpu.VMEM((NCHUNK, PIECE, CHUNK), BF16)
    wide = pltpu.VMEM((NCHUNK, PIECE, CHUNK), F32)
    return pl.pallas_call(
        output_kernel,
        out_shape=jax.ShapeDtypeStruct((PIECE, WIDTH), BF16),
        in_specs=[vmem, vmem],
        out_specs=vmem,
        scratch_shapes=[
            piece, piece, wide, piece, piece, piece, piece, piece, wide,
            pltpu.SemaphoreType.DMA((32,)),
            pltpu.SemaphoreType.DMA((32,)),
        ],
        compiler_params=pltpu.CompilerParams(
            collective_id=3, has_side_effects=True, vmem_limit_bytes=48 << 20
        ),
        name="output",
    )(mixed, w)


def on_device(tokens, w_query, key_value_weight, w_out, doc_lengths):
    blk_index = lax.axis_index("blk")
    positions = blk_index * BLK + jnp.arange(BLK, dtype=jnp.int32)
    ends = jnp.cumsum(doc_lengths)
    after = positions[:, None] >= ends[None, :]
    starts = jnp.sum(jnp.where(after, doc_lengths[None, :], 0), axis=1).astype(jnp.int32)
    half = HEAD // 2
    freqs = jnp.power(rope_base, -2.0 * jnp.arange(half, dtype=F32) / HEAD)
    angle = (positions - starts).astype(F32)[:, None] * freqs[None, :]
    cosine, sine = jnp.cos(angle), jnp.sin(angle)
    cos2 = jnp.concatenate([cosine, cosine], axis=1)
    sin2 = jnp.concatenate([-sine, sine], axis=1)
    mixed, head_rows = attention(
        tokens, w_query, key_value_weight.reshape(64, 256), w_out, cos2, sin2, starts[None, :]
    )
    return project_out(mixed, head_rows.reshape(512, WIDTH))


def solution(mesh):
    return jax.shard_map(
        on_device,
        mesh=mesh,
        in_specs=(
            P(("blk", "heads"), None),
            P("blk", "heads"),
            P("blk", None, "heads"),
            P(("heads", "blk"), None),
            P(),
        ),
        out_specs=P(("blk", "heads"), None),
        check_vma=False,
    )
```

```python
import functools

import jax
import jax.numpy as jnp
from jax import lax
from jax.experimental import pallas as pl
from jax.experimental.pallas import tpu as pltpu
from jax.sharding import PartitionSpec as P

MESH = pl.DeviceIdType.MESH
BF16 = jnp.bfloat16
F32 = jnp.float32

HEAD = 128
QH = 4
BLK = 512
PIECE = 128
WIDTH = 4096
NX, NZ, NYL = 4, 8, 2
norm_epsilon = 1e-05
rope_base = 500000.0
masked_score = -1e30
LOG2E = 1.4426950408889634


class Place:
    def __init__(self):
        h = lax.axis_index("heads")
        b = lax.axis_index("blk")
        self.h, self.b = h, b
        self.yh, self.c = lax.div(h, 2), lax.rem(h, 2)
        self.yl = lax.div(b, NX * NZ)
        self.z = lax.rem(lax.div(b, NX), NZ)
        self.x = lax.rem(b, NX)
        self.row = b - self.x
        self.xs = [lax.rem(self.x + k, NX) for k in range(NX)]
        self.zs = [lax.rem(self.z + k, NZ) for k in range(NZ)]
        self.xp = (h, self.row + self.xs[1])
        self.xm = (h, self.row + self.xs[3])
        base = b - self.z * NX
        self.zp = (h, base + self.zs[1] * NX)
        self.zm = (h, base + self.zs[7] * NX)
        self.yf = (h, lax.rem(b + NX * NZ, 2 * NX * NZ))
        self.core = (h + 1 - 2 * self.c, b)
        y = 2 * self.yh + self.yl
        inner = lax.rem(b, NX * NZ)
        self.yp = self.at_y(lax.rem(y + 1, 4), inner)
        self.ym = self.at_y(lax.rem(y + 3, 4), inner)
        self.far = lax.rem(h + 2, 4)
        self.nextrow = (h, lax.rem(b + NX, 64))
        self.prevrow = (h, lax.rem(b + 60, 64))

    def at_y(self, y, inner):
        return (2 * lax.div(y, 2) + self.c, NX * NZ * lax.rem(y, 2) + inner)


def meet(devices):
    barrier = pltpu.get_barrier_semaphore()
    for device in devices:
        pl.semaphore_signal(barrier, inc=1, device_id=device, device_id_type=MESH)
    pl.semaphore_wait(barrier, len(devices))


class Sends:
    def __init__(self, send_sem, recv_sem):
        self.send_sem, self.recv_sem, self.made, self.count = send_sem, recv_sem, [], 0

    def make(self, src, dst, device):
        i = self.count
        self.count += 1
        return pltpu.make_async_remote_copy(
            src_ref=src,
            dst_ref=dst,
            send_sem=self.send_sem.at[i],
            recv_sem=self.recv_sem.at[i],
            device_id=device,
            device_id_type=MESH,
        )

    def start(self, src, dst, device):
        copy = self.make(src, dst, device)
        copy.start()
        self.made.append(copy)
        return copy

    def same(self, ref, device):
        return self.start(ref, ref, device)

    def drain(self):
        for copy in self.made:
            copy.wait_send()


FACTOR = HEAD ** (-0.5) * LOG2E


def layer_kernel(
    docs, tokens_in, wq_in, wkv_in, wout_in, freqs, out,
    tokens, xbuf, ra, rb, wq, wkv, wout, cos, sin, start, raw, qt, kv, acc, high,
    w, mixed, give_far, take_far, own_far, sum_far, via, got, give_near, take_near, near_sum,
    copy_sem, send_sem, recv_sem,
):
    p = Place()
    x, z, yl, h = p.x, p.z, p.yl, p.h
    own = [
        pltpu.make_async_copy(wkv_in, wkv.at[yl, z, x], copy_sem.at[0]),
        pltpu.make_async_copy(wq_in, wq.at[yl, z, x], copy_sem.at[1]),
        pltpu.make_async_copy(tokens_in, tokens, copy_sem.at[2]),
        pltpu.make_async_copy(wout_in, wout.at[yl, z, x], copy_sem.at[3]),
    ]
    for copy in own:
        copy.start()
    meet([p.xp, p.xm, p.zp, p.zm, p.yp, p.ym, p.core, p.nextrow, p.prevrow])
    s = Sends(send_sem, recv_sem)

    def both(ref):
        return (s.same(ref, p.xp), s.same(ref, p.xm))

    def settle(pair):
        pair[0].wait_recv()
        pair[1].wait_recv()

    own[0].wait()
    y_kv = s.same(wkv.at[yl, z, x], p.yf)
    own[1].wait()
    y_q = s.same(wq.at[yl, z, x], p.yf)
    own[2].wait()

    def normalize(i, carry):
        rows = pl.ds(pl.multiple_of(i * 16, 16), 16)
        v = tokens[rows, :].astype(F32)
        mean = jnp.mean(v * v, axis=1, keepdims=True)
        xbuf[h, rows, :] = (v * lax.rsqrt(mean + norm_epsilon)).astype(BF16)
        return carry

    lax.fori_loop(0, PIECE // 16, normalize, 0)

    def bx_send(zz):
        return both(wq.at[:, zz, x])

    def bx_forward(zz, pair):
        pair[0].wait_recv()
        one = s.same(wq.at[0, zz, p.xs[3]], p.xp)
        pair[1].wait_recv()
        return (one, s.same(wq.at[1, zz, p.xs[1]], p.xm))

    def z_forward(pair, step, ref_of):
        pair[1].wait_recv()
        above = s.same(ref_of(p.zs[step]), p.zm)
        pair[0].wait_recv()
        below = s.same(ref_of(p.zs[NZ - step]), p.zp) if step < 3 else None
        return (below, above)

    def pick_b(zz):
        return wq.at[:, zz, x]

    def pick_a(zz):
        return wkv.at[:, zz]

    y_kv.wait_recv()
    ax = both(wkv.at[:, z, x])
    own[3].wait()
    w_side = both(wout.at[yl, z, x])
    y_q.wait_recv()
    bz = (s.same(wq.at[:, z, x], p.zp), s.same(wq.at[:, z, x], p.zm))
    rows0 = bx_send(z)
    act_core = s.same(xbuf.at[h], p.core)
    act = (
        s.start(xbuf.at[h, pl.ds(0, 64)], ra, p.yp),
        s.start(xbuf.at[h, pl.ds(64, 64)], rb, p.ym),
    )
    def first_of(position):
        first, end = jnp.zeros_like(position), 0
        for k in range(docs.shape[0]):
            end = end + docs[k]
            first = jnp.where(position >= end, end, first)
        return first

    start[...] = first_of(p.b * BLK + lax.broadcasted_iota(jnp.int32, (1, BLK), 1))

    def turn(t, carry):
        rows = pl.ds(pl.multiple_of(t * 64, 64), 64)
        position = p.b * BLK + t * 64 + lax.broadcasted_iota(jnp.int32, (64, HEAD), 0)
        angle = (position - first_of(position)).astype(F32) * freqs[...]
        cos[rows, :] = jnp.cos(angle)
        sine = jnp.sin(angle)
        left = lax.broadcasted_iota(jnp.int32, (64, HEAD), 1) < HEAD // 2
        sin[rows, :] = jnp.where(left, -sine, sine)
        return carry

    lax.fori_loop(0, BLK // 64, turn, 0)

    ax[0].wait_recv()
    ax_far0 = s.same(wkv.at[0, z, p.xs[3]], p.xp)
    ax[1].wait_recv()
    ax_far = (ax_far0, s.same(wkv.at[1, z, p.xs[1]], p.xm))
    w_side[0].wait_recv()
    w_far0 = s.same(wout.at[yl, z, p.xs[3], :, pl.ds(0, 2048)], p.xp)
    w_side[1].wait_recv()
    w_far = (w_far0, s.same(wout.at[yl, z, p.xs[1], :, pl.ds(2048, 2048)], p.xm))
    bz = z_forward(bz, 1, pick_b)
    rows1 = (bx_send(p.zs[7]), bx_send(p.zs[1]))
    settle(ax_far)
    az = (s.same(pick_a(z), p.zp), s.same(pick_a(z), p.zm))
    settle(w_far)
    w_y = []

    def w_up(zz):
        w_y.append(s.same(wout.at[yl, zz], p.yf))

    def w_from_below(step):
        nonlocal w_below
        w_below.wait_recv()
        zz = p.zs[NZ - step]
        if step < 3:
            w_below = s.same(wout.at[yl, zz], p.zp)
        w_up(zz)

    bz = z_forward(bz, 2, pick_b)
    rows2 = (bx_send(p.zs[6]), bx_send(p.zs[2]))
    far0 = bx_forward(z, rows0)
    act[0].wait_recv()
    relay0 = s.start(ra, xbuf.at[p.ym[0], pl.ds(0, 64)], p.yp)
    act[1].wait_recv()
    relay1 = s.start(rb, xbuf.at[p.yp[0], pl.ds(64, 64)], p.ym)
    w_up(z)
    az = z_forward(az, 1, pick_a)
    w_below = s.same(wout.at[yl, z], p.zp)
    bz = z_forward(bz, 3, pick_b)
    rows3 = (bx_send(p.zs[5]), bx_send(p.zs[3]))
    far1 = (bx_forward(p.zs[7], rows1[0]), bx_forward(p.zs[1], rows1[1]))
    az = z_forward(az, 2, pick_a)
    w_from_below(1)
    bz[1].wait_recv()
    rows4 = bx_send(p.zs[4])
    far2 = (bx_forward(p.zs[6], rows2[0]), bx_forward(p.zs[2], rows2[1]))
    settle((relay0, relay1))
    act_far = s.same(xbuf.at[p.far], p.core)
    az = z_forward(az, 3, pick_a)
    w_above = s.same(wout.at[yl, z], p.zm)

    def w_from_above(step):
        nonlocal w_above
        w_above.wait_recv()
        zz = p.zs[step]
        if step < 4:
            w_above = s.same(wout.at[yl, zz], p.zm)
        w_up(zz)

    far3 = (bx_forward(p.zs[5], rows3[0]), bx_forward(p.zs[3], rows3[1]))
    az[1].wait_recv()
    settle((act_core, act_far))
    w_from_below(2)

    def left_of(k):
        return xbuf[:, :, pl.ds(pl.multiple_of(k * 512, 512), 512)].reshape(BLK, 512)

    def multiply_kv(k, carry):
        right = wkv[lax.div(k, 4), pl.ds(2 * lax.rem(k, 4), 2)].reshape(512, 256)
        raw[:, 512:] += jnp.dot(left_of(k), right, preferred_element_type=F32)
        return carry

    def multiply_q(k, carry):
        right = wq[lax.div(k, 4), pl.ds(2 * lax.rem(k, 4), 2)].reshape(512, 512)
        raw[:, :512] += jnp.dot(left_of(k), right, preferred_element_type=F32)
        return carry

    def rotated(rows, at):
        v = raw[rows, at : at + HEAD]
        return v * cos[rows, :] + pltpu.roll(v, HEAD // 2, 1) * sin[rows, :]

    raw[...] = jnp.zeros_like(raw)
    lax.fori_loop(0, 8, multiply_kv, 0)
    for t in range(4):
        rows = slice(t * PIECE, (t + 1) * PIECE)
        kv[0, x, :, rows] = raw[rows, 640:768].T.astype(BF16)
        kv[0, x, :, BLK + t * PIECE : BLK + (t + 1) * PIECE] = rotated(rows, 512).astype(BF16)
    far4 = bx_forward(p.zs[4], rows4)
    down = s.start(kv.at[0, x], kv.at[1, x], p.nextrow)
    side, far = {}, {}
    inner = (x >= 1) & (x <= 2)
    first_row = (x <= 2, x >= 1, x == 0, x == 3, x >= 2)
    last_row = (x >= 1, x <= 2, x == 3, x == 0, x <= 1)

    class Edge:
        def __init__(self, d, onward, back, behind, conditions):
            self.sends, self.takes, self.wraps, self.wrapped, self.passed = conditions
            self.copy = s.make(kv.at[d, x], kv.at[d, x], onward)
            self.wrap = s.make(kv.at[d, x], kv.at[d, x], back)
            self.onward = s.make(kv.at[d, behind], kv.at[d, behind], onward)

        def begin(self):
            pl.when(self.sends)(self.copy.start)
            pl.when(self.wraps)(self.wrap.start)

        def hand_on(self):
            pl.when(self.takes)(self.copy.wait_recv)
            pl.when(inner)(self.onward.start)

        def near(self):
            pl.when(self.wrapped)(self.wrap.wait_recv)

        def rest(self):
            pl.when(self.passed)(self.onward.wait_recv)

        def end(self):
            pl.when(self.sends)(self.copy.wait_send)
            pl.when(self.wraps)(self.wrap.wait_send)
            pl.when(inner)(self.onward.wait_send)

    top = Edge(0, p.xp, p.xm, p.xs[3], first_row)
    bottom = Edge(4, p.xm, p.xp, p.xs[1], last_row)
    top.begin()
    w_from_below(3)

    for pair in (far0, far1[0], far1[1], far2[0], far2[1], far3[0], far3[1], far4):
        settle(pair)
    lax.fori_loop(0, 8, multiply_q, 0)
    for j in range(QH):
        for t in range(4):
            rows = slice(t * PIECE, (t + 1) * PIECE)
            qt[:, j * BLK + t * PIECE : j * BLK + (t + 1) * PIECE] = (
                (rotated(rows, j * HEAD) * FACTOR).T.astype(BF16)
            )

    key_at = lax.broadcasted_iota(jnp.int32, (BLK, BLK), 0)

    def attend(d, xx, diagonal=False):
        first = start[...] - (p.row + xx - NX * d) * BLK
        keys = jnp.concatenate(
            [kv[d, xx, :, BLK + i * HEAD : BLK + (i + 1) * HEAD] for i in range(4)], axis=0
        )
        vals = jnp.concatenate([kv[d, xx, :, :BLK], jnp.ones((16, BLK), BF16)], axis=0)

        def scores(j):
            return jnp.dot(
                keys, qt[:, j * BLK : (j + 1) * BLK], preferred_element_type=F32
            )

        def finish(j, score):
            at = slice(j * BLK, (j + 1) * BLK)
            keep = key_at >= first
            if diagonal:
                keep &= key_at <= lax.broadcasted_iota(jnp.int32, (BLK, BLK), 1)
            score = jnp.where(keep, score, masked_score)
            new = jnp.max(score, axis=0, keepdims=True)
            if not diagonal:
                old = high[:, at]
                new = jnp.maximum(old, new)
            probs = jnp.exp2(score - new).astype(BF16)
            update = jnp.dot(vals, probs, preferred_element_type=F32)
            if not diagonal:
                update += acc[:, at] * jnp.exp2(old - new)
            acc[:, at] = update
            high[:, at] = new

        now = scores(0)
        for j in range(QH):
            later = scores(j + 1) if j + 1 < QH else None
            finish(j, now)
            now = later

    def take_down(d):
        nonlocal down
        down.wait_recv()
        if d < 4:
            down = s.start(kv.at[d, x], kv.at[d + 1, x], p.nextrow)
        if d < 4:
            side[d] = both(kv.at[d, x])
        else:
            bottom.begin()

    def take_side(d):
        side[d][0].wait_recv()
        one = s.same(kv.at[d, p.xs[3], pl.ds(0, 64)], p.xp)
        side[d][1].wait_recv()
        far[d] = (one, s.same(kv.at[d, p.xs[1], pl.ds(64, 64)], p.xm))

    def end_row(d):
        settle(far[d])

    def edge(k):
        xx = p.xs[k]
        attend(4 * lax.div(xx - x + 3, 4), xx)

    attend(0, x, diagonal=True)
    take_down(1)
    w_from_above(1)
    attend(1, x)
    take_down(2)
    top.hand_on()
    w_from_above(2)
    attend(2, x)
    take_side(1)
    attend(1, p.xs[3])
    attend(1, p.xs[1])
    take_down(3)
    w_from_above(3)
    attend(3, x)
    take_side(2)
    end_row(1)
    attend(1, p.xs[2])
    attend(2, p.xs[3])
    attend(2, p.xs[1])
    take_down(4)
    w_from_above(4)
    attend(4, x)
    take_side(3)
    end_row(2)
    attend(2, p.xs[2])
    attend(3, p.xs[3])
    attend(3, p.xs[1])
    bottom.hand_on()
    end_row(3)
    attend(3, p.xs[2])
    top.near()
    bottom.near()
    edge(3)
    edge(1)
    for copy in w_y:
        copy.wait_recv()

    def flatten(g, carry):
        rows = pl.ds(pl.multiple_of(g * 32, 32), 32)
        w[rows, :] = wout[lax.div(g, NZ), lax.rem(g, NZ)].reshape(32, WIDTH)
        return carry

    lax.fori_loop(0, NYL * NZ, flatten, 0)
    top.rest()
    bottom.rest()
    edge(2)

    other = h + 1 - 2 * p.c
    far_other = lax.rem(other + 2, 4)

    def piece(owner):
        return pl.ds(pl.multiple_of(owner * PIECE, PIECE), PIECE)

    def mix(owner):
        for j in range(QH):
            at = pl.ds(pl.multiple_of(j * BLK + owner * PIECE, PIECE), PIECE)
            part = acc[:HEAD, at] * (1.0 / acc[HEAD : HEAD + 1, at])
            mixed[piece(owner), j * HEAD : (j + 1) * HEAD] = part.T.astype(BF16)

    def times(owner, n):
        return jnp.dot(
            mixed[piece(owner), :], w[:, n * CHUNK : (n + 1) * CHUNK], preferred_element_type=F32
        )

    def toward(n):
        return p.yp if n % 2 == 0 else p.ym

    to_core, hops, near, last = [], [], [], []

    def combine(n):
        to_core[n].wait_recv()
        sum_far[n] = (own_far[n] + take_far[n].astype(F32)).astype(BF16)
        hops.append(s.start(sum_far.at[n], via.at[n], toward(n)))

    mix(far_other)
    mix(p.far)
    for n in range(NCHUNK):
        give_far[n] = times(far_other, n).astype(BF16)
        to_core.append(s.start(give_far.at[n], take_far.at[n], p.core))
        own_far[n] = times(p.far, n)
        if n >= 2:
            combine(n - 2)
    combine(NCHUNK - 2)
    combine(NCHUNK - 1)
    mix(other)
    mix(h)
    for n in range(NCHUNK):
        give_near[n] = times(other, n).astype(BF16)
        near.append(s.start(give_near.at[n], take_near.at[n], p.core))
        near_sum[n] = times(h, n)
    for n in range(NCHUNK):
        hops[n].wait_recv()
        last.append(s.start(via.at[n], got.at[n], toward(n)))
    for n in range(NCHUNK):
        near[n].wait_recv()
        near_sum[n] += take_near[n].astype(F32)
    for n in range(NCHUNK):
        last[n].wait_recv()
        out[:, n * CHUNK : (n + 1) * CHUNK] = (near_sum[n] + got[n].astype(F32)).astype(BF16)
    s.drain()
    top.end()
    bottom.end()


NCHUNK, CHUNK = 8, 512


def layer(docs, tokens, wq, wkv, wout, freqs):
    vmem = pl.BlockSpec(memory_space=pltpu.VMEM)
    hbm = pl.BlockSpec(memory_space=pl.ANY)
    piece = pltpu.VMEM((NCHUNK, PIECE, CHUNK), BF16)
    wide = pltpu.VMEM((NCHUNK, PIECE, CHUNK), F32)
    return pl.pallas_call(
        layer_kernel,
        out_shape=jax.ShapeDtypeStruct((PIECE, WIDTH), BF16),
        in_specs=[pl.BlockSpec(memory_space=pltpu.SMEM), hbm, hbm, hbm, hbm, vmem],
        out_specs=vmem,
        scratch_shapes=[
            pltpu.VMEM((PIECE, WIDTH), BF16),
            pltpu.VMEM((4, PIECE, WIDTH), BF16),
            pltpu.VMEM((64, WIDTH), BF16),
            pltpu.VMEM((64, WIDTH), BF16),
            pltpu.VMEM((NYL, NZ, NX, 64, 512), BF16),
            pltpu.VMEM((NYL, NZ, NX, 64, 256), BF16),
            pltpu.VMEM((NYL, NZ, NX, 8, WIDTH), BF16),
            pltpu.VMEM((BLK, HEAD), F32),
            pltpu.VMEM((BLK, HEAD), F32),
            pltpu.VMEM((1, BLK), jnp.int32),
            pltpu.VMEM((BLK, 768), F32),
            pltpu.VMEM((HEAD, QH * BLK), BF16),
            pltpu.VMEM((5, NX, HEAD, 2 * BLK), BF16),
            pltpu.VMEM((HEAD + 16, QH * BLK), F32),
            pltpu.VMEM((1, QH * BLK), F32),
            pltpu.VMEM((BLK, WIDTH), BF16),
            pltpu.VMEM((BLK, QH * HEAD), BF16),
            piece, piece, wide, piece, piece, piece, piece, piece, wide,
            pltpu.SemaphoreType.DMA((4,)),
            pltpu.SemaphoreType.DMA((160,)),
            pltpu.SemaphoreType.DMA((160,)),
        ],
        compiler_params=pltpu.CompilerParams(
            collective_id=1, has_side_effects=True, vmem_limit_bytes=60 << 20
        ),
        name="layer",
    )(docs, tokens, wq, wkv, wout, freqs)


def on_device(tokens, w_query, key_value_weight, w_out, doc_lengths):
    half = HEAD // 2
    freqs = jnp.power(rope_base, -2.0 * jnp.arange(half, dtype=F32) / HEAD)
    freqs = jnp.concatenate([freqs, freqs])[None, :]
    return layer(
        doc_lengths, tokens, w_query, key_value_weight.reshape(64, 256), w_out, freqs
    )


def solution(mesh):
    return jax.shard_map(
        on_device,
        mesh=mesh,
        in_specs=(
            P(("blk", "heads"), None),
            P("blk", "heads"),
            P("blk", None, "heads"),
            P(("heads", "blk"), None),
            P(),
        ),
        out_specs=P(("blk", "heads"), None),
        check_vma=False,
    )
```
